32 devices in a mesh: tile: 16 (over z, y, x), lev: 2 (over core).
Axes of the slice: x: 2, y: 2, z: 4, core: 2. Of those that a mesh axis runs over, the one named last changes fastest.
Arguments:
- increments: bfloat16 [136, 256, 1024], P('lev', 'tile'), may hold values from -30 to 30
- projection: bfloat16 [80, 136], replicated, may hold values from -0.5 to 0.5
- helmholtz: float32 [80], P('lev'), may hold values from 0.05 to 4
Outputs:
- solution: float32 [80, 256, 1024], P('lev', 'tile')
- residual: float32 [80, 256, 1024], P('lev', 'tile')
The draws below stay inside these ranges and needn't reach their ends.
All inputs are finite; a program needn't handle non-finite values.
Results may differ from the reference program's by a relative error of at most 0.00075.
Values may be sent and summed in bfloat16 or wider, within the bound.
A program may use at most 192 MiB of HBM per device.

```python
import math
import jax
import jax.numpy as jnp
import numpy as np
from jax import lax

LEVELS = 136
MODES = 80
S = 4
BLOCKS = 2
NY = 1024
NX = 256


def lowpass(field):
    for repeat in range(2):
        field = 0.25 * (jnp.roll(field, 1, 1) + 2.0 * field + jnp.roll(field, -1, 1))
        field = 0.25 * (jnp.roll(field, 1, 2) + 2.0 * field + jnp.roll(field, -1, 2))
    return field


def draw_increments(key, part):
    key_base = jax.random.fold_in(key, 11)
    key_one, key_two = jax.random.split(key_base, 2)
    row_frac = (jnp.arange(NX, dtype=jnp.float32) / NX)[None, :, None]
    base = jnp.clip(jax.random.normal(key_one, (LEVELS, NX, NY), jnp.float32), -6.0, 6.0)
    smooth = lowpass(jnp.clip(jax.random.normal(key_two, (LEVELS, NX, NY), jnp.float32), -6.0, 6.0))
    values = base + 10.0 * row_frac * smooth
    return jnp.clip(values, -30.0, 30.0).astype(jnp.bfloat16)


def levels(stream_key, dims, cuts, least, high):
    loudness, own = 1.0, jax.random.fold_in(stream_key, 6)
    for axis_at, blocks in cuts:
        steps = jnp.exp(jax.random.uniform(jax.random.fold_in(own, axis_at), (blocks,), jnp.float32, least / len(cuts), high / len(cuts)))
        loudness = loudness * jnp.repeat(steps, dims[axis_at] // blocks).reshape([-1 if axis == axis_at else 1 for axis in range(len(dims))])
    return loudness


def normal_values(key, extent, deviation, bound, held_as=jnp.bfloat16):
    entries = deviation * jax.random.normal(key, extent, jnp.float32)
    return jnp.clip(entries, min=-bound, max=bound).astype(held_as)


def setup_inputs(seed: int = 0) -> dict:
    streams_of = jax.random.split(jax.random.key(seed), 4)
    increments = draw_increments(jax.random.fold_in(streams_of[3], 71), 0)
    projection = normal_values(streams_of[1], (MODES, LEVELS), LEVELS ** -0.5, 0.5)
    helmholtz = jnp.clip(jnp.exp(math.log(4.0) - 4.3820266 * jax.random.uniform(streams_of[2], (MODES,), jnp.float32) ** levels(streams_of[2], (MODES,), ((0, 2),), -0.2, 0.2)), 0.05, 4.0)
    return dict(increments=increments, projection=projection, helmholtz=helmholtz)


highest = lax.Precision.HIGHEST


def stencil(field, weight):
    padded = jnp.pad(field, 1)
    beside_all = padded[2:, 1:-1] + padded[:-2, 1:-1] + padded[1:-1, 2:] + padded[1:-1, :-2]
    return weight * beside_all


def shift_matrix():
    width = 2 * S + 1
    table = np.zeros((width, width), np.float32)
    for index in range(S):
        table[index + 1, index] = 1.0
    for index in range(S - 1):
        table[S + 2 + index, S + 1 + index] = 1.0
    return jnp.asarray(table, jnp.float32)


def quadratic(gram, left, right):
    return jnp.dot(left, jnp.dot(gram, right, precision=highest), precision=highest)


def solve_mode(inputs):
    rhs, weight = inputs
    width = 2 * S + 1
    shifter = shift_matrix()
    solution = jnp.zeros_like(rhs)
    resid = rhs
    direction = rhs
    for block_index in range(BLOCKS):
        vectors = [direction]
        current = direction
        for power_index in range(S):
            current = stencil(current, weight)
            vectors.append(current)
        vectors.append(resid)
        current = resid
        for power_index in range(S - 1):
            current = stencil(current, weight)
            vectors.append(current)
        basis = jnp.stack(vectors).reshape(width, -1)
        gram = jnp.dot(basis, basis.T, precision=highest)
        p_coef = jnp.zeros((width,), jnp.float32).at[0].set(1.0)
        r_coef = jnp.zeros((width,), jnp.float32).at[S + 1].set(1.0)
        x_coef = jnp.zeros((width,), jnp.float32)
        squares = quadratic(gram, r_coef, r_coef)
        for step_index in range(S):
            moved = p_coef - jnp.dot(shifter, p_coef, precision=highest)
            alpha = squares / quadratic(gram, p_coef, moved)
            x_coef = x_coef + alpha * p_coef
            r_coef = r_coef - alpha * moved
            fresh = quadratic(gram, r_coef, r_coef)
            p_coef = r_coef + (fresh / squares) * p_coef
            squares = fresh
        solution = solution + jnp.dot(x_coef, basis, precision=highest).reshape(rhs.shape)
        resid = jnp.dot(r_coef, basis, precision=highest).reshape(rhs.shape)
        direction = jnp.dot(p_coef, basis, precision=highest).reshape(rhs.shape)
    return solution, resid


def reference(increments, projection, helmholtz):
    flat = increments.reshape(LEVELS, NX * NY)
    modal = jnp.dot(projection, flat, preferred_element_type=jnp.float32).reshape(MODES, NX, NY)
    weights = 1.0 / (4.0 + helmholtz)
    solution, resid = lax.map(solve_mode, (modal, weights))
    return solution, resid
```

```python
import functools

import jax
import jax.numpy as jnp
from jax import lax
from jax.experimental import pallas as pl
from jax.experimental.pallas import tpu as pltpu
from jax.sharding import PartitionSpec as P

S = 4
HALO = 2 * S
POWER = 13
UNROLL = 1
SUB = 8
LANE = 128
MESH = pl.DeviceIdType.MESH
f32 = jnp.float32
bf16 = jnp.bfloat16


def stage_groups(count):
    groups = []
    while count > 1:
        size = 4 if count % 4 == 0 else (2 if count % 2 == 0 else count)
        groups.append(size)
        count //= size
    return groups


def encode(value, scale):
    a = value * scale
    a4 = (a * a) * (a * a)
    return ((a4 * a4) * (a4 * a)).astype(bf16)


def decode(code, scale):
    code = code.astype(f32)
    size = jnp.exp(jnp.log(jnp.maximum(jnp.abs(code), 2.0 ** -126)) * (1.0 / POWER)) * (1.0 / scale)
    return jnp.where(code > 0.0, size, jnp.where(code < 0.0, -size, 0.0))


def spread(tile, times):
    return jnp.concatenate([tile] * times, axis=1)


def add(left, right):
    if left is None:
        return right
    if right is None:
        return left
    return left + right


def scaled(factor, vector):
    return [None if entry is None else factor * entry for entry in vector]


def added(left, right):
    return [add(a, b) for a, b in zip(left, right)]


def minus(left, right):
    result = []
    for a, b in zip(left, right):
        if b is None:
            result.append(a)
        elif a is None:
            result.append(-b)
        else:
            result.append(a - b)
    return result


def form(gram, left, right):
    total = None
    for a, left_entry in enumerate(left):
        if left_entry is None:
            continue
        inner = None
        for b, right_entry in enumerate(right):
            if right_entry is not None:
                inner = add(inner, gram(a, b) * right_entry)
        total = add(total, left_entry * inner)
    return total


def recurrence(gram, shift, p_coef, r_coef):
    x_coef = [None] * len(p_coef)
    squares = form(gram, r_coef, r_coef)
    for step in range(S):
        moved = minus(p_coef, shift(p_coef))
        alpha = squares / form(gram, p_coef, moved)
        x_coef = added(x_coef, scaled(alpha, p_coef))
        r_coef = minus(r_coef, scaled(alpha, moved))
        fresh = form(gram, r_coef, r_coef)
        p_coef = added(r_coef, scaled(fresh / squares, p_coef))
        squares = fresh
    return x_coef, r_coef, p_coef


def kernel(tiles, levs, groups, rows, modes, cells, levels, inc_ref, proj_ref, helm_ref, sol_ref, res_ref,
           x_all, wide, fields, dirs, res0, extra, total, out_buf, in_buf, weights, sums, coefs, grams,
           local_sems, swap_send, swap_recv, halo_send, halo_recv, gram_send, gram_recv):
    tile = lax.axis_index("tile")
    lev = lax.axis_index("lev")
    part = inc_ref.shape[0]
    across = cells // LANE
    parts_m = modes // SUB
    barrier = pltpu.get_barrier_semaphore()

    stage_peers = []
    stride = 1
    for size in groups:
        digit = lax.rem(lax.div(tile, stride), size)
        base = tile - digit * stride
        peers = []
        for j in range(1, size):
            peers.append(base + lax.rem(digit + j, size) * stride)
        stage_peers.append((digit, peers))
        stride *= size

    count = 0
    for j in range(1, levs):
        pl.semaphore_signal(barrier, 1, device_id=(tile, lax.rem(lev + j, levs)), device_id_type=MESH)
        count += 1
    for peer in (lax.rem(tile + 1, tiles), lax.rem(tile + tiles - 1, tiles)):
        pl.semaphore_signal(barrier, 1, device_id=(peer, lev), device_id_type=MESH)
        count += 1
    for digit, peers in stage_peers:
        for peer in peers:
            pl.semaphore_signal(barrier, 1, device_id=(peer, lev), device_id_type=MESH)
            count += 1

    local = pltpu.make_async_copy(inc_ref, x_all.at[0], local_sems.at[0])
    local.start()

    proj = proj_ref[...].astype(f32)
    own = proj[0:modes]
    for j in range(1, levs):
        own = jnp.where(lev == j, proj[j * modes:(j + 1) * modes], own)
    own_levels = levels // levs
    groups_l = [own[:, j * own_levels:(j + 1) * own_levels] for j in range(levs)]
    depth = part
    col_e = lax.broadcasted_iota(jnp.int32, (own_levels, depth), 1)
    row_e = lax.broadcasted_iota(jnp.int32, (own_levels, depth), 0) * rows
    onehot = jnp.where((col_e >= row_e) & (col_e < row_e + rows), 1.0, 0.0).astype(bf16)
    col_w = lax.rem(lax.broadcasted_iota(jnp.int32, (2 * modes, depth), 1), rows)
    second = jnp.where(lax.broadcasted_iota(jnp.int32, (2 * modes, depth), 0) >= modes, 1, 0)
    pick = col_w - second

    def widen(position):
        chosen = groups_l[position]
        for j in range(1, levs):
            chosen = jnp.where(lev == j, groups_l[(j + position) % levs], chosen)
        twice = jnp.concatenate([chosen, chosen], axis=0).astype(bf16)
        repeated = jnp.dot(twice, onehot, preferred_element_type=f32)
        for pair in range(rows // 2):
            wide[position, pair * 2 * modes:(pair + 1) * 2 * modes, :] = jnp.where(
                pick == 2 * pair, repeated, 0.0).astype(bf16)

    widen(0)
    pl.semaphore_wait(barrier, count)
    swaps = []
    for j in range(1, levs):
        copy = pltpu.make_async_remote_copy(
            src_ref=inc_ref, dst_ref=x_all.at[levs - j], send_sem=swap_send.at[j - 1],
            recv_sem=swap_recv.at[j - 1], device_id=(tile, lax.rem(lev + j, levs)), device_id_type=MESH)
        copy.start()
        swaps.append(copy)

    diag = lax.broadcasted_iota(jnp.int32, (modes, modes), 0) == lax.broadcasted_iota(jnp.int32, (modes, modes), 1)
    helm = jnp.sum(jnp.where(diag, jnp.broadcast_to(helm_ref[...], (modes, modes)), 0.0), axis=1, keepdims=True)
    weight = jnp.broadcast_to(1.0 / (4.0 + helm), (modes, LANE))
    weights[0] = weight
    weights[1] = jnp.where(tile > 0, weight, 0.0)
    weights[2] = jnp.where(tile < tiles - 1, weight, 0.0)
    sums[...] = jnp.zeros_like(sums)

    base_row = HALO
    field = fields.at[0]
    block = 2 * LANE if cells % (2 * LANE) == 0 else LANE

    def project_part(position):
        def project(index, carry):
            cols = pl.ds(pl.multiple_of(index * block, block), block)
            got = jnp.dot(wide[position], x_all[position, :, cols], preferred_element_type=f32)
            got = got.reshape(rows, modes, block)
            if position:
                got = field[base_row:base_row + rows, :, cols] + got
            field[base_row:base_row + rows, :, cols] = got
            return carry

        lax.fori_loop(0, cells // block, project, 0)

    local.wait()
    project_part(0)
    for j in range(1, levs):
        widen(j)
    for j in range(1, levs):
        swaps[j - 1].wait()
    for j in range(1, levs):
        project_part(j)

    slots = HALO // 2
    scale = 2.0 ** 9.7 / (0.5 * 30.0 * levels)

    def own_pair(side, pair):
        first = 2 * pair if side == 0 else rows - 2 - 2 * pair
        return field[base_row + first:base_row + first + 2].reshape(2 * modes, cells)

    def halo_copy(side, slot):
        peer = lax.rem(tile + tiles - 1, tiles) if side == 0 else lax.rem(tile + 1, tiles)
        return pltpu.make_async_remote_copy(
            src_ref=out_buf.at[side, slot], dst_ref=in_buf.at[side, slot], send_sem=halo_send.at[side, slot],
            recv_sem=halo_recv.at[side, slot], device_id=(peer, lev), device_id_type=MESH)

    for slot in range(slots):
        for side in range(2):
            out_buf[side, slot] = encode(own_pair(side, slot), scale)

        @pl.when(tile > 0)
        def _(slot=slot):
            halo_copy(0, slot).start()

        @pl.when(tile < tiles - 1)
        def _(slot=slot):
            halo_copy(1, slot).start()

    has = {0: tile < tiles - 1, 1: tile > 0}

    def take(side, pair):
        first = base_row + rows + 2 * pair if side == 0 else base_row - 2 - 2 * pair

        @pl.when(has[side])
        def _():
            halo_copy(side, pair).wait_recv()
            field[first:first + 2] = decode(in_buf[side, pair], scale).reshape(2, modes, cells)

        @pl.when(jnp.logical_not(has[side]))
        def _():
            field[first:first + 2] = jnp.zeros((2, modes, cells), f32)

    lane = lax.broadcasted_iota(jnp.int32, (SUB, LANE), 1)
    first_lane = lane == 0
    last_lane = lane == LANE - 1
    nothing = jnp.zeros((SUB, LANE), f32)

    def beside(tile_row):
        pieces = [tile_row[:, j * LANE:(j + 1) * LANE] for j in range(across)]
        right = [pltpu.roll(piece, 1, 1) for piece in pieces]
        left = [pltpu.roll(piece, LANE - 1, 1) for piece in pieces]
        result = []
        for j in range(across):
            low = jnp.where(first_lane, right[j - 1] if j else nothing, right[j])
            high = jnp.where(last_lane, left[j + 1] if j + 1 < across else nothing, left[j])
            result.append(low + high)
        return jnp.concatenate(result, axis=1)

    def fold(product):
        pieces = [product[:, j * LANE:(j + 1) * LANE] for j in range(across)]
        while len(pieces) > 1:
            pieces = [pieces[i] + pieces[i + 1] if i + 1 < len(pieces) else pieces[i] for i in range(0, len(pieces), 2)]
        return pieces[0]

    def over_rows(low, high, body):
        if high <= low:
            return
        if high - low == 1:
            body(low)
            return

        def step(index, carry):
            body(index)
            return carry

        lax.fori_loop(low, high, step, 0, unroll=UNROLL if (high - low) % UNROLL == 0 else 1)

    def apply(src, src_off, dst, dst_off, low, high, pairs=(), which=0):
        def body(row):
            for m in range(parts_m):
                at = slice(m * SUB, (m + 1) * SUB)
                here = src[row + src_off, at, :]
                around = src[row + src_off - 1, at, :] + src[row + src_off + 1, at, :] + beside(here)
                fresh = spread(weights[which, at, :], across) * around
                dst[row + dst_off, at, :] = fresh
                cache = {"src": here, "dst": fresh}
                for slot, left, right in pairs:
                    values = []
                    for operand in (left, right):
                        if isinstance(operand, str):
                            values.append(cache[operand])
                        else:
                            ref, off = operand
                            values.append(ref[row + off, at, :])
                    sums[slot, at, :] = sums[slot, at, :] + fold(values[0] * values[1])

        over_rows(low, high, body)

    def apply_all(src, src_off, dst, dst_off, wide_by, pairs):
        apply(src, src_off, dst, dst_off, -wide_by, 0, which=1)
        apply(src, src_off, dst, dst_off, 0, rows, pairs)
        apply(src, src_off, dst, dst_off, rows, rows + wide_by, which=2)

    def power_pairs(power):
        found = [(2 * power - 1, "src", "dst"), (2 * power, "dst", "dst")]
        if power == 1:
            found.append((0, "src", "src"))
        return found

    for power in range(1, S + 1):
        apply(fields.at[power - 1], HALO, fields.at[power], HALO, power, rows - power, power_pairs(power))
    for pair in range(S // 2):
        for side in range(2):
            take(side, pair)
    for power in range(1, S + 1):
        src, dst = fields.at[power - 1], fields.at[power]
        found = power_pairs(power)
        apply(src, HALO, dst, HALO, power - S, 0, which=1)
        apply(src, HALO, dst, HALO, 0, power, found)
        apply(src, HALO, dst, HALO, rows - power, rows, found)
        apply(src, HALO, dst, HALO, rows, rows + S - power, which=2)

    def packed(number):
        lanes = lax.broadcasted_iota(jnp.int32, (modes, LANE), 1)
        table = jnp.zeros((modes, LANE), f32)
        for slot in range(number):
            table = jnp.where(lanes == slot, jnp.sum(sums[slot], axis=1, keepdims=True), table)
        return table

    def gram_copies(block_index, stage):
        digit, peers = stage_peers[stage]
        size = groups[stage]
        sends = []
        for j in range(1, size):
            sends.append(pltpu.make_async_remote_copy(
                src_ref=grams.at[block_index, stage, digit], dst_ref=grams.at[block_index, stage, digit],
                send_sem=gram_send.at[block_index, stage, j - 1], recv_sem=gram_recv.at[block_index, stage, digit],
                device_id=(peers[j - 1], lev), device_id_type=MESH))
        return sends

    def gram_start(block_index, stage, table):
        grams[block_index, stage, stage_peers[stage][0]] = table
        for copy in gram_copies(block_index, stage):
            copy.start()

    def gram_finish(block_index, stage):
        digit, peers = stage_peers[stage]
        size = groups[stage]
        for copy in gram_copies(block_index, stage):
            copy.wait_send()
        for j in range(1, size):
            sender = lax.rem(digit + j, size)
            pltpu.make_async_remote_copy(
                src_ref=grams.at[block_index, stage, sender], dst_ref=grams.at[block_index, stage, sender],
                send_sem=gram_send.at[block_index, stage, j - 1], recv_sem=gram_recv.at[block_index, stage, sender],
                device_id=(peers[j - 1], lev), device_id_type=MESH).wait_recv()
        table = grams[block_index, stage, 0]
        for j in range(1, size):
            table = table + grams[block_index, stage, j]
        return table

    def column(table, slot):
        return jnp.broadcast_to(table[:, slot:slot + 1], (modes, LANE))

    def finish_all(block_index, table):
        for stage in range(len(groups)):
            if stage:
                gram_start(block_index, stage, table)
            table = gram_finish(block_index, stage)
        return table

    table = packed(2 * S + 1)
    gram_start(0, 0, table)

    for pair in range(S // 2, HALO // 2):
        for side in range(2):
            take(side, pair)
    for power in range(1, S + 1):
        src, dst = fields.at[power - 1], fields.at[power]
        apply(src, HALO, dst, HALO, power - HALO, power - S, which=1)
        apply(src, HALO, dst, HALO, rows + S - power, rows + HALO - power, which=2)
    sums[...] = jnp.zeros_like(sums)

    table = finish_all(0, table)
    moments = [column(table, slot) for slot in range(2 * S + 1)]
    one = jnp.ones((modes, LANE), f32)
    start = [one] + [None] * S
    x_coef, r_coef, p_coef = recurrence(
        lambda a, b: moments[a + b], lambda vector: [None] + vector[:-1], start, start)

    def keep(lists):
        position, kept = 0, []
        for entries in lists:
            places = []
            for index, entry in enumerate(entries):
                if entry is not None:
                    coefs[position] = entry
                    places.append((index, position))
                    position += 1
            kept.append(places)
        return kept

    def combined(places, values, at):
        result = None
        for index, position in places:
            result = add(result, spread(coefs[position, at, :], across) * values[index])
        return result

    x_at, r_at, p_at = keep([x_coef, r_coef, p_coef])

    def mix(low, high, inside):
        def body(row):
            for m in range(parts_m):
                at = slice(m * SUB, (m + 1) * SUB)
                values = [fields[power, row + HALO, at, :] for power in range(S + 1)]
                if inside:
                    total[row, at, :] = combined(x_at, values, at)
                res0[row + S, at, :] = combined(r_at, values, at)
                dirs[row + S, at, :] = combined(p_at, values, at)

        over_rows(low, high, body)

    mix(-S, 0, False)
    mix(0, rows, True)
    mix(rows, rows + S, False)

    d_refs = [(dirs, S)] + [(fields.at[power], HALO) for power in range(1, S + 1)]
    r_refs = [(res0, S), (fields.at[0], HALO)] + [(extra.at[power], S) for power in range(S - 2)]
    md, mr, cross = 0, 2 * S + 1, 4 * S
    for power in range(1, S + 1):
        found = [(md + 2 * power - 1, "src", "dst"), (md + 2 * power, "dst", "dst")]
        if power == 1:
            found.append((md, "src", "src"))
        apply_all(*d_refs[power - 1], *d_refs[power], S - power, found)
    for power in range(1, S):
        found = [(mr + 2 * power - 1, "src", "dst"), (mr + 2 * power, "dst", "dst"),
                 (cross + 2 * power, d_refs[power], "dst"), (cross + 2 * power + 1, d_refs[power + 1], "dst")]
        if power == 1:
            found += [(mr, "src", "src"), (cross, d_refs[0], "src"), (cross + 1, d_refs[1], "src")]
        apply_all(*r_refs[power - 1], *r_refs[power], S - 1 - power, found)

    number = 6 * S
    table = packed(number)
    gram_start(1, 0, table)
    table = finish_all(1, table)
    moments = [column(table, slot) for slot in range(number)]

    def gram(a, b):
        if a > S and b > S:
            return moments[mr + a + b - 2 * S - 2]
        if a > S or b > S:
            return moments[cross + a + b - S - 1]
        return moments[md + a + b]

    def shift(vector):
        return [None] + vector[:S] + [None] + vector[S + 1:2 * S]

    x_coef, r_coef, p_coef = recurrence(
        gram, shift, [one] + [None] * (2 * S), [None] * (S + 1) + [one] + [None] * (S - 1))
    x_at, r_at = keep([x_coef, r_coef])

    def last(row):
        for m in range(parts_m):
            at = slice(m * SUB, (m + 1) * SUB)
            values = [ref[row + off, at, :] for ref, off in d_refs + r_refs]
            total[row, at, :] = total[row, at, :] + combined(x_at, values, at)
            dirs[row + S, at, :] = combined(r_at, values, at)

    chunk = rows // 2
    writes = []
    for index in range(2):
        over_rows(index * chunk, (index + 1) * chunk, last)
        rng = pl.ds(index * chunk, chunk)
        copy = pltpu.make_async_copy(total.at[rng], sol_ref.at[rng], local_sems.at[1 + 2 * index])
        copy.start()
        writes.append(copy)
        copy = pltpu.make_async_copy(dirs.at[pl.ds(S + index * chunk, chunk)], res_ref.at[rng], local_sems.at[2 + 2 * index])
        copy.start()
        writes.append(copy)

    for slot in range(slots):
        @pl.when(tile > 0)
        def _(slot=slot):
            halo_copy(0, slot).wait_send()

        @pl.when(tile < tiles - 1)
        def _(slot=slot):
            halo_copy(1, slot).wait_send()
    for copy in writes:
        copy.wait()


def shards(increments, projection, helmholtz):
    tiles, levs = lax.axis_size("tile"), lax.axis_size("lev")
    own_levels, rows, cells = increments.shape
    modes = projection.shape[0] // levs
    levels = own_levels * levs
    groups = stage_groups(tiles)
    most = max(groups)
    slots = HALO // 2
    vmem = pltpu.VMEM
    dma = pltpu.SemaphoreType.DMA
    scratch = [
        vmem((levs, own_levels * rows, cells), bf16),
        vmem((levs, rows * modes, own_levels * rows), bf16),
        vmem((S + 1, rows + 2 * HALO, modes, cells), f32),
        vmem((rows + 2 * S, modes, cells), f32),
        vmem((rows + 2 * S, modes, cells), f32),
        vmem((S - 2, rows + 2 * S, modes, cells), f32),
        vmem((rows, modes, cells), f32),
        vmem((2, slots, 2 * modes, cells), bf16),
        vmem((2, slots, 2 * modes, cells), bf16),
        vmem((3, modes, LANE), f32),
        vmem((6 * S, modes, LANE), f32),
        vmem((6 * S, modes, LANE), f32),
        vmem((2, len(groups), most, modes, LANE), f32),
        dma((5,)),
        dma((levs - 1,)),
        dma((levs - 1,)),
        dma((2, slots)),
        dma((2, slots)),
        dma((2, len(groups), most)),
        dma((2, len(groups), most)),
    ]
    shape = jax.ShapeDtypeStruct((rows, modes, cells), f32)
    solved, resid = pl.pallas_call(
        functools.partial(kernel, tiles, levs, groups, rows, modes, cells, levels),
        out_shape=(shape, shape),
        in_specs=[pl.BlockSpec(memory_space=pl.ANY), pl.BlockSpec(memory_space=pltpu.VMEM),
                  pl.BlockSpec(memory_space=pltpu.VMEM)],
        out_specs=(pl.BlockSpec(memory_space=pl.ANY), pl.BlockSpec(memory_space=pl.ANY)),
        scratch_shapes=scratch,
        compiler_params=pltpu.CompilerParams(collective_id=0, has_side_effects=True, vmem_limit_bytes=67000000),
    )(increments.reshape(own_levels * rows, cells), projection, helmholtz.reshape(1, modes))
    return jnp.transpose(solved, (1, 0, 2)), jnp.transpose(resid, (1, 0, 2))


def solution(mesh):
    in_specs = (P("lev", "tile", None), P(), P("lev"))
    out_specs = (P("lev", "tile", None), P("lev", "tile", None))
    return jax.shard_map(shards, mesh=mesh, in_specs=in_specs, out_specs=out_specs, check_vma=False)
```
